32 devices in a mesh: span: 32 (over z, y, x, core).
Axes of the slice: x: 2, y: 2, z: 4, core: 2. Of those that a mesh axis runs over, the one named last changes fastest.
Arguments:
- random_slabs: bfloat16 [1024, 4, 3, 2048], P('span'), may hold values from -6 to 6
- span_weights: float32 [513], replicated, may hold values from 0.1 to 2
- wall_filter: bfloat16 [2048, 2048], replicated, may hold values from -0.125 to 0.125
- prev_state: float32 [1024, 3, 2048], P('span'), may hold values from -6 to 6
- time_scale: float32 [3, 2048], replicated, may hold values from 1 to 32
- mean_velocity: float32 [2048], replicated, may hold values from 0 to 2
- lund_diag: float32 [3, 2048], replicated, may hold values from 0.3 to 3
- lund_off: float32 [3, 2048], replicated, may hold values from -1 to 1
Outputs:
- velocity: bfloat16 [1024, 4, 3, 2048], P('span')
- new_state: float32 [1024, 3, 2048], P('span')
The draws below stay inside these ranges and needn't reach their ends.
All inputs are finite; a program needn't handle non-finite values.
Results may differ from the reference program's by a relative error of at most 0.0051.
Values may be sent and summed in bfloat16 or wider, within the bound.
A program may use at most 128 MiB of HBM per device.

```python
import math
import jax
import jax.numpy as jnp
from jax import lax

NY = 2048
PLANES = 4
NZ = 1024
HALF = 256


def draw_span_weights(key, part):
    offsets = jnp.arange(-HALF, HALF + 1).astype(jnp.float32)
    spread = jnp.float32(HALF)
    envelope = jnp.exp(-jnp.pi * offsets * offsets / (2.0 * spread * spread))
    factor = jnp.exp(jax.random.uniform(key, (2 * HALF + 1,), jnp.float32, math.log(0.5), math.log(2.0)))
    return envelope * factor


def steps_of(rng, shape, cuts, smallest, top_value):
    factor_of, own = 1.0, jax.random.fold_in(rng, 6)
    for position, shards_of in cuts:
        steps = jnp.exp(jax.random.uniform(jax.random.fold_in(own, position), (shards_of,), jnp.float32, smallest / len(cuts), top_value / len(cuts)))
        factor_of = factor_of * jnp.repeat(steps, shape[position] // shards_of).reshape([-1 if axis == position else 1 for axis in range(len(shape))])
    return factor_of


def bell_draw(rng, extent, scale, bound, shards=(), kind=jnp.bfloat16):
    level = steps_of(rng, extent, shards, -0.22, 0.18) if shards else 1.0
    result = jax.random.normal(rng, extent, jnp.float32) * scale * level
    return jnp.minimum(jnp.maximum(result, -bound), bound).astype(kind)


def setup_inputs(seed: int = 0) -> dict:
    key_list = jax.random.split(jax.random.key(seed), 9)
    return {
        "random_slabs": bell_draw(key_list[0], (NZ, PLANES, 3, NY), 1.0, 6.0, ((0, 32),)),
        "span_weights": draw_span_weights(jax.random.fold_in(key_list[8], 71), 0),
        "wall_filter": bell_draw(key_list[2], (NY, NY), NY ** -0.5, 0.125),
        "prev_state": bell_draw(key_list[3], (NZ, 3, NY), 1.0, 6.0, ((0, 32),), jnp.float32),
        "time_scale": jnp.clip(jnp.exp(jax.random.uniform(key_list[4], (3, NY), jnp.float32, math.log(1.0), math.log(32.0))), 1.0, 32.0),
        "mean_velocity": jnp.clip(jax.random.uniform(key_list[5], (NY,), jnp.float32, 0.0, 2.0), 0.0, 2.0),
        "lund_diag": jnp.clip(jnp.exp(jax.random.uniform(key_list[6], (3, NY), jnp.float32, math.log(0.3), math.log(3.0))), 0.3, 3.0),
        "lund_off": jnp.clip(jax.random.uniform(key_list[7], (3, NY), jnp.float32, -1.0, 1.0), -1.0, 1.0),
    }


def normalized_taps(span_weights):
    norm = jnp.sqrt(jnp.sum(span_weights * span_weights))
    return (span_weights / norm).astype(jnp.bfloat16)

def reference(random_slabs, span_weights, wall_filter, prev_state, time_scale, mean_velocity, lund_diag, lund_off):
    total = random_slabs.shape[0]
    taps = lax.optimization_barrier(normalized_taps(span_weights)).astype(jnp.float32)
    middle = jnp.zeros((total - 2 * HALF - 1,), jnp.float32)
    kernel = jnp.concatenate([taps[HALF:], middle, taps[:HALF]])
    kernel_hat = jnp.conj(jnp.fft.rfft(kernel))
    slabs = random_slabs.reshape(total, PLANES * 3, NY).transpose(1, 0, 2)
    wall_wide = wall_filter.astype(jnp.float32)

    def one_slab(slab):
        spectrum = jnp.fft.rfft(slab.astype(jnp.float32), axis=0)
        spanned = jnp.fft.irfft(spectrum * kernel_hat[:, None], n=total, axis=0)
        spanned = lax.optimization_barrier(spanned.astype(jnp.bfloat16)).astype(jnp.float32)
        return jnp.dot(spanned, wall_wide.T, precision=lax.Precision.HIGHEST)
    filtered = lax.map(one_slab, slabs).reshape(PLANES, 3, total, NY)
    decay = jnp.exp(-jnp.pi / (2.0 * time_scale))[:, None, :]
    inject = jnp.sqrt(1.0 - jnp.exp(-jnp.pi / time_scale))[:, None, :]

    def advance(state, plane):
        state = decay * state + inject * plane
        return (state, state)
    final, fluct = lax.scan(advance, prev_state.transpose(1, 0, 2), filtered)
    along = fluct[:, 0]
    normal = fluct[:, 1]
    spanwise = fluct[:, 2]
    first = mean_velocity + lund_diag[0] * along
    second = lund_off[0] * along + lund_diag[1] * normal
    third = lund_off[1] * along + lund_off[2] * normal + lund_diag[2] * spanwise
    velocity = jnp.stack([first, second, third], axis=1).astype(jnp.bfloat16)
    return (velocity.transpose(2, 0, 1, 3), final.transpose(1, 0, 2))
```

```python
import functools

import jax
import jax.numpy as jnp
from jax import lax
from jax.experimental import pallas as pl
from jax.experimental.pallas import tpu as pltpu
from jax.sharding import PartitionSpec as P

LANES = 256
MESH = pl.DeviceIdType.MESH


def peer_of(step, me, count):
    away = count // 2 + (1 - 2 * (step % 2)) * ((step + 1) // 2)
    return lax.rem(me + away, count)


def exchange_kernel(
    count,
    rows,
    width,
    pairs,
    parts,
    slim,
    reach,
    x_ref,
    taps_ref,
    wall_ref,
    prev_ref,
    scale_ref,
    mean_ref,
    diag_ref,
    off_ref,
    vel_ref,
    state_ref,
    wide,
    summed,
    back,
    band,
    wall,
    decay,
    inject,
    wall_sem,
    out_sem,
    in_sem,
    back_out_sem,
    back_in_sem,
):
    me = lax.axis_index("span")
    per = width // slim
    group = pairs // parts
    blocks = count * rows // reach

    wall_copy = pltpu.make_async_copy(wall_ref, wall, wall_sem)
    wall_copy.start()

    barrier = pltpu.get_barrier_semaphore()

    @pl.loop(0, count - 1)
    def _(step):
        pl.semaphore_signal(
            barrier, inc=1, device_id=(peer_of(step, me, count),), device_id_type=MESH
        )

    pl.semaphore_wait(barrier, count - 1)

    def columns(part, owner):
        slot = part * count + owner
        start = pl.multiple_of((slot % per) * slim, slim)
        return slot // per, pl.ds(start, slim)

    for part in range(parts):

        @pl.loop(0, count - 1)
        def _(step):
            peer = peer_of(step, me, count)
            pair, span = columns(part, peer)
            pltpu.make_async_remote_copy(
                src_ref=x_ref.at[pair, :, span],
                dst_ref=wide.at[part, me],
                send_sem=out_sem.at[part],
                recv_sem=in_sem.at[part],
                device_id=(peer,),
                device_id_type=MESH,
            ).start()

        pair, span = columns(part, me)
        pltpu.make_async_copy(x_ref.at[pair, :, span], wide.at[part, me], in_sem.at[part]).start()

    weights = taps_ref[...]
    taps = weights / jnp.sqrt(jnp.sum(weights * weights))
    tall = jnp.broadcast_to(taps, (16, 3 * reach))
    line = lax.broadcasted_iota(jnp.int32, (16, 3 * reach), 0)
    for bit in range(4):
        tall = jnp.where((line // (1 << bit)) % 2 == 1, pltpu.roll(tall, 1 << bit, 1), tall)

    @pl.loop(0, reach // 16)
    def _(step):
        first = pl.multiple_of(step * 16, 16)
        rolled = pltpu.roll(tall, first, 1)
        band[pl.ds(first, 16), :] = rolled.astype(jnp.bfloat16)

    decay[...] = jnp.exp(-jnp.pi / (2.0 * scale_ref[...]))
    inject[...] = jnp.sqrt(1.0 - jnp.exp(-jnp.pi / scale_ref[...]))
    state_ref[...] = prev_ref[...]

    for part in range(parts):
        pltpu.make_async_copy(wide.at[part], wide.at[part], in_sem.at[part]).wait()
        share = reach // rows
        for block in range(blocks):
            total = jnp.zeros((reach, slim), jnp.float32)
            for shift in range(3):
                source = (block - 1 + shift) % blocks
                chunk = wide[part, source * share : (source + 1) * share].reshape(reach, slim)
                total += jnp.dot(
                    band[:, shift * reach : (shift + 1) * reach],
                    chunk,
                    preferred_element_type=jnp.float32,
                )
            summed[part, block * share : (block + 1) * share] = total.astype(
                jnp.bfloat16
            ).reshape(share, rows, slim)

        pair, span = columns(part, me)

        @pl.loop(0, count - 1)
        def _(step):
            peer = peer_of(step, me, count)
            pltpu.make_async_remote_copy(
                src_ref=summed.at[part, peer],
                dst_ref=back.at[pair, :, span],
                send_sem=back_out_sem.at[part],
                recv_sem=back_in_sem.at[part],
                device_id=(peer,),
                device_id_type=MESH,
            ).start()

        pltpu.make_async_copy(
            summed.at[part, me], back.at[pair, :, span], back_in_sem.at[part]
        ).start()

    wall_copy.wait()
    tile = min(256, width)
    for part in range(parts):
        mine = back.at[part * group : (part + 1) * group]
        pltpu.make_async_copy(mine, mine, back_in_sem.at[part]).wait()

        @pl.loop(0, width // tile)
        def _(step):
            at = pl.ds(pl.multiple_of(step * tile, tile), tile)
            filtered = lax.dot_general(
                back[part * group : (part + 1) * group].reshape(group * rows, width),
                wall[at, :],
                (((1,), (1,)), ((), ())),
                preferred_element_type=jnp.float32,
            ).reshape(group, rows, tile)
            for local in range(group):
                pair = part * group + local
                component = pair % 3
                one = pl.ds(component, 1)
                new = decay[one, at] * state_ref[component, :, at] + inject[one, at] * filtered[local]
                state_ref[component, :, at] = new
                if component == 0:
                    value = mean_ref[:, at] + diag_ref[0:1, at] * new
                elif component == 1:
                    value = off_ref[0:1, at] * state_ref[0, :, at] + diag_ref[1:2, at] * new
                else:
                    value = (
                        off_ref[1:2, at] * state_ref[0, :, at]
                        + off_ref[2:3, at] * state_ref[1, :, at]
                        + diag_ref[2:3, at] * new
                    )
                vel_ref[pair, :, at] = value.astype(jnp.bfloat16)

    for part in range(parts):
        sent = wide.at[part, 0 : count - 1]
        pltpu.make_async_copy(sent, sent, out_sem.at[part]).wait()
        pltpu.make_async_copy(sent, sent, back_out_sem.at[part]).wait()


def fits(count, rows, pairs, width, reach, slim):
    columns = pairs * width
    return (
        columns % (count * slim) == 0
        and (count * slim) % width == 0
        and width % slim == 0
        and rows % 16 == 0
        and reach % rows == 0
        and reach % 128 == 0
        and count * rows % reach == 0
        and count * rows // reach >= 3
    )


def exchanged(
    random_slabs,
    span_weights,
    wall_filter,
    prev_state,
    time_scale,
    mean_velocity,
    lund_diag,
    lund_off,
):
    count = lax.axis_size("span")
    rows, planes, kinds, width = random_slabs.shape
    pairs = planes * kinds
    reach = (span_weights.shape[0] - 1) // 2
    slim = LANES
    parts = pairs * width // (count * slim)
    x = random_slabs.transpose(1, 2, 0, 3).reshape(pairs, rows, width)
    padded = jnp.pad(span_weights, (0, 3 * reach - span_weights.shape[0])).reshape(1, 3 * reach)
    in_vmem = pl.BlockSpec(memory_space=pltpu.VMEM)
    velocity, state = pl.pallas_call(
        functools.partial(exchange_kernel, count, rows, width, pairs, parts, slim, reach),
        out_shape=(
            jax.ShapeDtypeStruct((pairs, rows, width), jnp.bfloat16),
            jax.ShapeDtypeStruct((kinds, rows, width), jnp.float32),
        ),
        in_specs=[in_vmem, in_vmem, pl.BlockSpec(memory_space=pl.ANY)] + [in_vmem] * 5,
        out_specs=(in_vmem, in_vmem),
        scratch_shapes=[
            pltpu.VMEM((parts, count, rows, slim), jnp.bfloat16),
            pltpu.VMEM((parts, count, rows, slim), jnp.bfloat16),
            pltpu.VMEM((pairs, rows, width), jnp.bfloat16),
            pltpu.VMEM((reach, 3 * reach), jnp.bfloat16),
            pltpu.VMEM((width, width), jnp.bfloat16),
            pltpu.VMEM((kinds, width), jnp.float32),
            pltpu.VMEM((kinds, width), jnp.float32),
            pltpu.SemaphoreType.DMA,
            pltpu.SemaphoreType.DMA((parts,)),
            pltpu.SemaphoreType.DMA((parts,)),
            pltpu.SemaphoreType.DMA((parts,)),
            pltpu.SemaphoreType.DMA((parts,)),
        ],
        compiler_params=pltpu.CompilerParams(collective_id=0, has_side_effects=True),
    )(
        x,
        padded,
        wall_filter,
        prev_state.transpose(1, 0, 2),
        time_scale,
        mean_velocity.reshape(1, width),
        lund_diag,
        lund_off,
    )
    velocity = velocity.reshape(planes, kinds, rows, width).transpose(2, 0, 1, 3)
    return velocity, state.transpose(1, 0, 2)


def from_partner(value, axis, bit):
    return lax.ppermute(value, axis, [(i, i ^ 1 << bit) for i in range(lax.axis_size(axis))])


def band_matrix(taps, height):
    reach = taps.shape[0]
    padded = jnp.concatenate([taps, jnp.zeros((height,), taps.dtype)])
    length = reach + height
    tiled = jnp.tile(padded, height)[: height * (length - 1)]
    return tiled.reshape(height, length - 1)


def butterfly(held, forward):
    count = lax.axis_size("span")
    device = lax.axis_index("span")
    levels = count.bit_length() - 1
    for level in range(levels - 1, -1, -1):
        groups, inner_first, targets, inner_last = held.shape
        halves = held.reshape(groups, inner_first, 2, targets // 2, inner_last)
        lower = halves[:, :, 0]
        higher = halves[:, :, 1]
        upper = device >> level & 1 == 1
        kept = jnp.where(upper, higher, lower)
        given = jnp.where(upper, lower, higher)
        if forward:
            taken = from_partner(given, "span", level)
        else:
            taken = from_partner(given, "span", level)
        first = jnp.where(upper, taken, kept)
        second = jnp.where(upper, kept, taken)
        held = jnp.stack([first, second], axis=1).reshape(
            groups * 2, inner_first, targets // 2, inner_last
        )
    return held


def body(
    random_slabs,
    span_weights,
    wall_filter,
    prev_state,
    time_scale,
    mean_velocity,
    lund_diag,
    lund_off,
):
    rows = random_slabs.shape[0]
    planes = random_slabs.shape[1]
    width = random_slabs.shape[3]
    columns = planes * 3 * width
    half = (span_weights.shape[0] - 1) // 2
    if fits(lax.axis_size("span"), rows, planes * 3, width, half, LANES):
        return exchanged(
            random_slabs,
            span_weights,
            wall_filter,
            prev_state,
            time_scale,
            mean_velocity,
            lund_diag,
            lund_off,
        )
    flat = random_slabs.reshape(rows, columns)
    scaling = jnp.sqrt(jnp.sum(span_weights * span_weights))
    taps = (span_weights / scaling).astype(jnp.bfloat16)
    reach = (span_weights.shape[0] - 1) // 2
    count = lax.axis_size("span")
    slim = columns // count
    held = butterfly(flat.reshape(1, rows, count, slim), True)
    total = rows * count
    whole = held.reshape(total, slim)
    height = min(512, total)
    matrix = band_matrix(taps, height)
    wrapped = jnp.concatenate([whole[total - reach :], whole, whole[:reach]], axis=0)

    def one_block(start):
        window = lax.dynamic_slice_in_dim(wrapped, start, height + 2 * reach, 0)
        return jnp.dot(matrix, window, preferred_element_type=jnp.float32)

    starts = jnp.arange(total // height) * height
    summed_cols = lax.map(one_block, starts).reshape(total, slim)
    rounded = summed_cols.astype(jnp.bfloat16)
    returned = butterfly(rounded.reshape(1, 1, count, rows * slim), False)
    spanned = returned.reshape(count, rows, slim).transpose(1, 0, 2).reshape(rows, planes, 3, width)
    filtered = lax.dot_general(
        spanned, wall_filter, (((3,), (1,)), ((), ())), preferred_element_type=jnp.float32
    )
    decay = jnp.exp(-jnp.pi / (2.0 * time_scale))
    inject = jnp.sqrt(1.0 - jnp.exp(-jnp.pi / time_scale))
    state = prev_state
    outputs = []
    for plane in range(planes):
        state = decay * state + inject * filtered[:, plane]
        along = state[:, 0]
        normal = state[:, 1]
        spanwise = state[:, 2]
        first = mean_velocity + lund_diag[0] * along
        second = lund_off[0] * along + lund_diag[1] * normal
        third = lund_off[1] * along + lund_off[2] * normal + lund_diag[2] * spanwise
        outputs.append(jnp.stack([first, second, third], axis=1).astype(jnp.bfloat16))
    velocity = jnp.stack(outputs, axis=1)
    return (velocity, state)


def solution(mesh):
    placed = (P("span", None, None, None), P(), P(), P("span", None, None), P(), P(), P(), P())
    return jax.shard_map(
        body,
        mesh=mesh,
        in_specs=placed,
        out_specs=(P("span", None, None, None), P("span", None, None)),
        check_vma=False,
    )
```

```python
import functools

import jax
import jax.numpy as jnp
from jax import lax
from jax.experimental import pallas as pl
from jax.experimental.pallas import tpu as pltpu
from jax.sharding import PartitionSpec as P

LANES = 256
MESH = pl.DeviceIdType.MESH


def peer_of(step, me, count):
    away = count // 2 + (1 - 2 * (step % 2)) * ((step + 1) // 2)
    return lax.rem(me + away, count)


def exchange_kernel(
    count,
    rows,
    width,
    pairs,
    parts,
    slim,
    reach,
    slab_ref,
    taps_ref,
    wall_ref,
    prev_ref,
    scale_ref,
    mean_ref,
    diag_ref,
    off_ref,
    vel_ref,
    state_ref,
    x_ref,
    wide,
    summed,
    back,
    band,
    wall,
    early,
    decay,
    inject,
    wall_sem,
    out_sem,
    in_sem,
    back_out_sem,
    back_in_sem,
):
    me = lax.axis_index("span")
    per = width // slim
    group = pairs // parts
    blocks = count * rows // reach

    wall_copy = pltpu.make_async_copy(wall_ref, wall, wall_sem)
    wall_copy.start()

    barrier = pltpu.get_barrier_semaphore()

    @pl.loop(0, count - 1)
    def _(step):
        pl.semaphore_signal(
            barrier, inc=1, device_id=(peer_of(step, me, count),), device_id_type=MESH
        )

    def relayout(part):
        for pair in range(part * group, (part + 1) * group):
            x_ref[pair] = slab_ref[:, pair % 3, pair // 3, :]

    relayout(0)
    pl.semaphore_wait(barrier, count - 1)

    half = count // 2
    side = per // 2
    ours = me // half

    def columns(part, owner):
        place = owner % half
        start = pl.multiple_of((owner // half * side + place % side) * slim, slim)
        return part * group + place // side, pl.ds(start, slim)

    for part in range(parts):
        if part:
            relayout(part)

        @pl.loop(0, count - 1)
        def _(step):
            peer = peer_of(step, me, count)
            pair, span = columns(part, peer)
            pltpu.make_async_remote_copy(
                src_ref=x_ref.at[pair, :, span],
                dst_ref=wide.at[part, me],
                send_sem=out_sem.at[part],
                recv_sem=in_sem.at[part],
                device_id=(peer,),
                device_id_type=MESH,
            ).start()

        pair, span = columns(part, me)
        pltpu.make_async_copy(x_ref.at[pair, :, span], wide.at[part, me], in_sem.at[part]).start()

    weights = jnp.concatenate(
        [taps_ref[...], jnp.zeros((3 * reach - taps_ref.shape[0],), jnp.float32)]
    ).reshape(1, 3 * reach)
    taps = weights / jnp.sqrt(jnp.sum(weights * weights))
    tall = jnp.broadcast_to(taps, (16, 3 * reach))
    line = lax.broadcasted_iota(jnp.int32, (16, 3 * reach), 0)
    for bit in range(4):
        tall = jnp.where((line // (1 << bit)) % 2 == 1, pltpu.roll(tall, 1 << bit, 1), tall)

    @pl.loop(0, reach // 16)
    def _(step):
        first = pl.multiple_of(step * 16, 16)
        rolled = pltpu.roll(tall, first, 1)
        band[pl.ds(first, 16), :] = rolled.astype(jnp.bfloat16)

    decay[...] = jnp.exp(-jnp.pi / (2.0 * scale_ref[...]))
    inject[...] = jnp.sqrt(1.0 - jnp.exp(-jnp.pi / scale_ref[...]))
    state_ref[...] = prev_ref[...]

    for part in range(parts):
        pltpu.make_async_copy(wide.at[part], wide.at[part], in_sem.at[part]).wait()
        share = reach // rows
        for block in range(blocks):
            total = jnp.zeros((reach, slim), jnp.float32)
            for shift in range(3):
                source = (block - 1 + shift) % blocks
                chunk = wide[part, source * share : (source + 1) * share].reshape(reach, slim)
                total += jnp.dot(
                    band[:, shift * reach : (shift + 1) * reach],
                    chunk,
                    preferred_element_type=jnp.float32,
                )
            summed[part, block * share : (block + 1) * share] = total.astype(
                jnp.bfloat16
            ).reshape(share, rows, slim)

        pair, span = columns(part, me)

        @pl.loop(0, count - 1)
        def _(step):
            peer = peer_of(step, me, count)
            pltpu.make_async_remote_copy(
                src_ref=summed.at[part, peer],
                dst_ref=back.at[pair, :, span],
                send_sem=back_out_sem.at[part],
                recv_sem=back_in_sem.at[part, (peer // half + ours) % 2],
                device_id=(peer,),
                device_id_type=MESH,
            ).start()

        pltpu.make_async_copy(
            summed.at[part, me], back.at[pair, :, span], back_in_sem.at[part, 0]
        ).start()

    def finish(part, at, filtered):
        for local in range(group):
            pair = part * group + local
            component = pair % 3
            one = pl.ds(component, 1)
            new = decay[one, at] * state_ref[component, :, at] + inject[one, at] * filtered[local]
            state_ref[component, :, at] = new
            if component == 0:
                value = mean_ref[:, at] + diag_ref[0:1, at] * new
            elif component == 1:
                value = off_ref[0:1, at] * state_ref[0, :, at] + diag_ref[1:2, at] * new
            else:
                value = (
                    off_ref[1:2, at] * state_ref[0, :, at]
                    + off_ref[2:3, at] * state_ref[1, :, at]
                    + diag_ref[2:3, at] * new
                )
            vel_ref[pair, :, at] = value.astype(jnp.bfloat16)

    wall_copy.wait()
    tile = min(256, width)
    for part in range(parts):
        held = back.at[part * group : (part + 1) * group]
        for far in range(2):
            first = pl.multiple_of((ours + far) % 2 * (width // 2), width // 2)
            span = pl.ds(first, width // 2)
            mine = held.at[:, :, 0 : width // 2]
            pltpu.make_async_copy(mine, mine, back_in_sem.at[part, far]).wait()
            if part < parts - 1 and far == 0:
                continue

            @pl.loop(0, width // tile)
            def _(step):
                at = pl.ds(pl.multiple_of(step * tile, tile), tile)
                reading = span if part == parts - 1 else slice(None)
                filtered = lax.dot_general(
                    held[:, :, reading].reshape(group * rows, -1),
                    wall[at, reading],
                    (((1,), (1,)), ((), ())),
                    preferred_element_type=jnp.float32,
                ).reshape(group, rows, tile)
                if far == 0:
                    early[:, :, at] = filtered
                else:
                    if part == parts - 1:
                        filtered += early[:, :, at]
                    finish(part, at, filtered)

    for part in range(parts):
        sent = wide.at[part, 0 : count - 1]
        pltpu.make_async_copy(sent, sent, out_sem.at[part]).wait()
        pltpu.make_async_copy(sent, sent, back_out_sem.at[part]).wait()


def fits(count, rows, pairs, width, reach, slim):
    columns = pairs * width
    return (
        columns % (count * slim) == 0
        and (count * slim) % width == 0
        and width % (2 * slim) == 0
        and count % 2 == 0
        and rows % 16 == 0
        and reach % rows == 0
        and reach % 128 == 0
        and count * rows % reach == 0
        and count * rows // reach >= 3
    )


def exchanged(
    random_slabs,
    span_weights,
    wall_filter,
    prev_state,
    time_scale,
    mean_velocity,
    lund_diag,
    lund_off,
):
    count = lax.axis_size("span")
    rows, planes, kinds, width = random_slabs.shape
    pairs = planes * kinds
    reach = (span_weights.shape[0] - 1) // 2
    slim = LANES
    parts = pairs * width // (count * slim)
    x = random_slabs.transpose(0, 2, 1, 3)
    in_vmem = pl.BlockSpec(memory_space=pltpu.VMEM)
    velocity, state = pl.pallas_call(
        functools.partial(exchange_kernel, count, rows, width, pairs, parts, slim, reach),
        out_shape=(
            jax.ShapeDtypeStruct((pairs, rows, width), jnp.bfloat16),
            jax.ShapeDtypeStruct((kinds, rows, width), jnp.float32),
        ),
        in_specs=[in_vmem, in_vmem, pl.BlockSpec(memory_space=pl.ANY)] + [in_vmem] * 5,
        out_specs=(in_vmem, in_vmem),
        scratch_shapes=[
            pltpu.VMEM((pairs, rows, width), jnp.bfloat16),
            pltpu.VMEM((parts, count, rows, slim), jnp.bfloat16),
            pltpu.VMEM((parts, count, rows, slim), jnp.bfloat16),
            pltpu.VMEM((pairs, rows, width), jnp.bfloat16),
            pltpu.VMEM((reach, 3 * reach), jnp.bfloat16),
            pltpu.VMEM((width, width), jnp.bfloat16),
            pltpu.VMEM((pairs // parts, rows, width), jnp.float32),
            pltpu.VMEM((kinds, width), jnp.float32),
            pltpu.VMEM((kinds, width), jnp.float32),
            pltpu.SemaphoreType.DMA,
            pltpu.SemaphoreType.DMA((parts,)),
            pltpu.SemaphoreType.DMA((parts,)),
            pltpu.SemaphoreType.DMA((parts,)),
            pltpu.SemaphoreType.DMA((parts, 2)),
        ],
        compiler_params=pltpu.CompilerParams(collective_id=0, has_side_effects=True),
    )(
        x,
        span_weights,
        wall_filter,
        prev_state.transpose(1, 0, 2),
        time_scale,
        mean_velocity.reshape(1, width),
        lund_diag,
        lund_off,
    )
    velocity = velocity.reshape(planes, kinds, rows, width).transpose(2, 0, 1, 3)
    return velocity, state.transpose(1, 0, 2)


def from_partner(value, axis, bit):
    return lax.ppermute(value, axis, [(i, i ^ 1 << bit) for i in range(lax.axis_size(axis))])


def band_matrix(taps, height):
    reach = taps.shape[0]
    padded = jnp.concatenate([taps, jnp.zeros((height,), taps.dtype)])
    length = reach + height
    tiled = jnp.tile(padded, height)[: height * (length - 1)]
    return tiled.reshape(height, length - 1)


def butterfly(held, forward):
    count = lax.axis_size("span")
    device = lax.axis_index("span")
    levels = count.bit_length() - 1
    for level in range(levels - 1, -1, -1):
        groups, inner_first, targets, inner_last = held.shape
        halves = held.reshape(groups, inner_first, 2, targets // 2, inner_last)
        lower = halves[:, :, 0]
        higher = halves[:, :, 1]
        upper = device >> level & 1 == 1
        kept = jnp.where(upper, higher, lower)
        given = jnp.where(upper, lower, higher)
        if forward:
            taken = from_partner(given, "span", level)
        else:
            taken = from_partner(given, "span", level)
        first = jnp.where(upper, taken, kept)
        second = jnp.where(upper, kept, taken)
        held = jnp.stack([first, second], axis=1).reshape(
            groups * 2, inner_first, targets // 2, inner_last
        )
    return held


def body(
    random_slabs,
    span_weights,
    wall_filter,
    prev_state,
    time_scale,
    mean_velocity,
    lund_diag,
    lund_off,
):
    rows = random_slabs.shape[0]
    planes = random_slabs.shape[1]
    width = random_slabs.shape[3]
    columns = planes * 3 * width
    half = (span_weights.shape[0] - 1) // 2
    if fits(lax.axis_size("span"), rows, planes * 3, width, half, LANES):
        return exchanged(
            random_slabs,
            span_weights,
            wall_filter,
            prev_state,
            time_scale,
            mean_velocity,
            lund_diag,
            lund_off,
        )
    flat = random_slabs.reshape(rows, columns)
    scaling = jnp.sqrt(jnp.sum(span_weights * span_weights))
    taps = (span_weights / scaling).astype(jnp.bfloat16)
    reach = (span_weights.shape[0] - 1) // 2
    count = lax.axis_size("span")
    slim = columns // count
    held = butterfly(flat.reshape(1, rows, count, slim), True)
    total = rows * count
    whole = held.reshape(total, slim)
    height = min(512, total)
    matrix = band_matrix(taps, height)
    wrapped = jnp.concatenate([whole[total - reach :], whole, whole[:reach]], axis=0)

    def one_block(start):
        window = lax.dynamic_slice_in_dim(wrapped, start, height + 2 * reach, 0)
        return jnp.dot(matrix, window, preferred_element_type=jnp.float32)

    starts = jnp.arange(total // height) * height
    summed_cols = lax.map(one_block, starts).reshape(total, slim)
    rounded = summed_cols.astype(jnp.bfloat16)
    returned = butterfly(rounded.reshape(1, 1, count, rows * slim), False)
    spanned = returned.reshape(count, rows, slim).transpose(1, 0, 2).reshape(rows, planes, 3, width)
    filtered = lax.dot_general(
        spanned, wall_filter, (((3,), (1,)), ((), ())), preferred_element_type=jnp.float32
    )
    decay = jnp.exp(-jnp.pi / (2.0 * time_scale))
    inject = jnp.sqrt(1.0 - jnp.exp(-jnp.pi / time_scale))
    state = prev_state
    outputs = []
    for plane in range(planes):
        state = decay * state + inject * filtered[:, plane]
        along = state[:, 0]
        normal = state[:, 1]
        spanwise = state[:, 2]
        first = mean_velocity + lund_diag[0] * along
        second = lund_off[0] * along + lund_diag[1] * normal
        third = lund_off[1] * along + lund_off[2] * normal + lund_diag[2] * spanwise
        outputs.append(jnp.stack([first, second, third], axis=1).astype(jnp.bfloat16))
    velocity = jnp.stack(outputs, axis=1)
    return (velocity, state)


def solution(mesh):
    placed = (P("span", None, None, None), P(), P(), P("span", None, None), P(), P(), P(), P())
    return jax.shard_map(
        body,
        mesh=mesh,
        in_specs=placed,
        out_specs=(P("span", None, None, None), P("span", None, None)),
        check_vma=False,
    )
```

```python
import functools

import jax
import jax.numpy as jnp
from jax import lax
from jax.experimental import pallas as pl
from jax.experimental.pallas import tpu as pltpu
from jax.sharding import PartitionSpec as P

LANES = 256
MESH = pl.DeviceIdType.MESH


def peer_of(step, me, count):
    away = count // 2 + (1 - 2 * (step % 2)) * ((step + 1) // 2)
    return lax.rem(me + away, count)


def exchange_kernel(
    count,
    rows,
    width,
    pairs,
    parts,
    slim,
    reach,
    slab_ref,
    taps_ref,
    wall_ref,
    prev_ref,
    scale_ref,
    mean_ref,
    diag_ref,
    off_ref,
    vel_ref,
    state_ref,
    x_ref,
    wide,
    summed,
    back,
    band,
    wall,
    early,
    decay,
    inject,
    wall_sem,
    out_sem,
    in_sem,
    back_out_sem,
    back_in_sem,
):
    me = lax.axis_index("span")
    per = width // slim
    group = pairs // parts
    blocks = count * rows // reach

    wall_copy = pltpu.make_async_copy(wall_ref, wall, wall_sem)
    wall_copy.start()

    barrier = pltpu.get_barrier_semaphore()

    @pl.loop(0, count - 1)
    def _(step):
        pl.semaphore_signal(
            barrier, inc=1, device_id=(peer_of(step, me, count),), device_id_type=MESH
        )

    def relayout(part):
        for pair in range(part * group, (part + 1) * group):
            x_ref[pair] = slab_ref[:, pair % 3, pair // 3, :]

    relayout(0)
    pl.semaphore_wait(barrier, count - 1)

    half = count // 2
    side = per // 2
    ours = me // half

    def columns(part, owner):
        place = owner % half
        start = pl.multiple_of((owner // half * side + place % side) * slim, slim)
        return part * group + place // side, pl.ds(start, slim)

    for part in range(parts):
        if part:
            relayout(part)

        @pl.loop(0, count - 1)
        def _(step):
            peer = peer_of(step, me, count)
            pair, span = columns(part, peer)
            pltpu.make_async_remote_copy(
                src_ref=x_ref.at[pair, :, span],
                dst_ref=wide.at[part, me],
                send_sem=out_sem.at[part],
                recv_sem=in_sem.at[part],
                device_id=(peer,),
                device_id_type=MESH,
            ).start()

        pair, span = columns(part, me)
        pltpu.make_async_copy(x_ref.at[pair, :, span], wide.at[part, me], in_sem.at[part]).start()

    weights = jnp.concatenate(
        [taps_ref[...], jnp.zeros((3 * reach - taps_ref.shape[0],), jnp.float32)]
    ).reshape(1, 3 * reach)
    taps = weights / jnp.sqrt(jnp.sum(weights * weights))
    tall = jnp.broadcast_to(taps, (16, 3 * reach))
    line = lax.broadcasted_iota(jnp.int32, (16, 3 * reach), 0)
    for bit in range(4):
        tall = jnp.where((line // (1 << bit)) % 2 == 1, pltpu.roll(tall, 1 << bit, 1), tall)

    @pl.loop(0, reach // 16)
    def _(step):
        first = pl.multiple_of(step * 16, 16)
        rolled = pltpu.roll(tall, first, 1)
        band[pl.ds(first, 16), :] = rolled.astype(jnp.bfloat16)

    decay[...] = jnp.exp(-jnp.pi / (2.0 * scale_ref[...]))
    inject[...] = jnp.sqrt(1.0 - jnp.exp(-jnp.pi / scale_ref[...]))
    state_ref[...] = prev_ref[...]

    for part in range(parts):
        pltpu.make_async_copy(wide.at[part], wide.at[part], in_sem.at[part]).wait()
        share = reach // rows
        for block in range(blocks):
            total = jnp.zeros((reach, slim), jnp.float32)
            for shift in range(3):
                source = (block - 1 + shift) % blocks
                chunk = wide[part, source * share : (source + 1) * share].reshape(reach, slim)
                total += jnp.dot(
                    band[:, shift * reach : (shift + 1) * reach],
                    chunk,
                    preferred_element_type=jnp.float32,
                )
            summed[part, block * share : (block + 1) * share] = total.astype(
                jnp.bfloat16
            ).reshape(share, rows, slim)

        pair, span = columns(part, me)

        @pl.loop(0, count - 1)
        def _(step):
            peer = peer_of(step, me, count)
            pltpu.make_async_remote_copy(
                src_ref=summed.at[part, peer],
                dst_ref=back.at[pair, :, span],
                send_sem=back_out_sem.at[part],
                recv_sem=back_in_sem.at[part, (peer // half + ours) % 2],
                device_id=(peer,),
                device_id_type=MESH,
            ).start()

        pltpu.make_async_copy(
            summed.at[part, me], back.at[pair, :, span], back_in_sem.at[part, 0]
        ).start()

    def finish(part, at, filtered):
        for local in range(group):
            pair = part * group + local
            component = pair % 3
            one = pl.ds(component, 1)
            new = decay[one, at] * state_ref[component, :, at] + inject[one, at] * filtered[local]
            state_ref[component, :, at] = new
            if component == 0:
                value = mean_ref[:, at] + diag_ref[0:1, at] * new
            elif component == 1:
                value = off_ref[0:1, at] * state_ref[0, :, at] + diag_ref[1:2, at] * new
            else:
                value = (
                    off_ref[1:2, at] * state_ref[0, :, at]
                    + off_ref[2:3, at] * state_ref[1, :, at]
                    + diag_ref[2:3, at] * new
                )
            vel_ref[pair, :, at] = value.astype(jnp.bfloat16)

    wall_copy.wait()
    tile = min(256, width)
    for part in range(parts):
        held = back.at[part * group : (part + 1) * group]
        for far in range(2):
            first = pl.multiple_of((ours + far) % 2 * (width // 2), width // 2)
            span = pl.ds(first, width // 2)
            mine = held.at[:, :, 0 : width // 2]
            pltpu.make_async_copy(mine, mine, back_in_sem.at[part, far]).wait()
            if part < parts - 1 and far == 0:
                continue

            @pl.loop(0, width // tile)
            def _(step):
                at = pl.ds(pl.multiple_of(step * tile, tile), tile)
                reading = span if part == parts - 1 else slice(None)
                filtered = lax.dot_general(
                    held[:, :, reading].reshape(group * rows, -1),
                    wall[at, reading],
                    (((1,), (1,)), ((), ())),
                    preferred_element_type=jnp.float32,
                ).reshape(group, rows, tile)
                if far == 0:
                    early[:, :, at] = filtered
                else:
                    if part == parts - 1:
                        filtered += early[:, :, at]
                    finish(part, at, filtered)

    for part in range(parts):
        sent = wide.at[part, 0 : count - 1]
        pltpu.make_async_copy(sent, sent, out_sem.at[part]).wait()
        pltpu.make_async_copy(sent, sent, back_out_sem.at[part]).wait()


def fits(count, rows, pairs, width, reach, slim):
    columns = pairs * width
    return (
        columns % (count * slim) == 0
        and (count * slim) % width == 0
        and width % (2 * slim) == 0
        and count % 2 == 0
        and rows % 16 == 0
        and reach % rows == 0
        and reach % 128 == 0
        and count * rows % reach == 0
        and count * rows // reach >= 3
    )


def exchanged(
    random_slabs,
    span_weights,
    wall_filter,
    prev_state,
    time_scale,
    mean_velocity,
    lund_diag,
    lund_off,
):
    count = lax.axis_size("span")
    rows, planes, kinds, width = random_slabs.shape
    pairs = planes * kinds
    reach = (span_weights.shape[0] - 1) // 2
    slim = LANES
    parts = pairs * width // (count * slim)
    x = random_slabs.transpose(0, 2, 1, 3)
    in_vmem = pl.BlockSpec(memory_space=pltpu.VMEM)
    velocity, state = pl.pallas_call(
        functools.partial(exchange_kernel, count, rows, width, pairs, parts, slim, reach),
        out_shape=(
            jax.ShapeDtypeStruct((pairs, rows, width), jnp.bfloat16),
            jax.ShapeDtypeStruct((kinds, rows, width), jnp.float32),
        ),
        in_specs=[in_vmem, in_vmem, pl.BlockSpec(memory_space=pltpu.HBM)] + [in_vmem] * 5,
        out_specs=(in_vmem, in_vmem),
        scratch_shapes=[
            pltpu.VMEM((pairs, rows, width), jnp.bfloat16),
            pltpu.VMEM((parts, count, rows, slim), jnp.bfloat16),
            pltpu.VMEM((parts, count, rows, slim), jnp.bfloat16),
            pltpu.VMEM((pairs, rows, width), jnp.bfloat16),
            pltpu.VMEM((reach, 3 * reach), jnp.bfloat16),
            pltpu.VMEM((width, width), jnp.bfloat16),
            pltpu.VMEM((pairs // parts, rows, width), jnp.float32),
            pltpu.VMEM((kinds, width), jnp.float32),
            pltpu.VMEM((kinds, width), jnp.float32),
            pltpu.SemaphoreType.DMA,
            pltpu.SemaphoreType.DMA((parts,)),
            pltpu.SemaphoreType.DMA((parts,)),
            pltpu.SemaphoreType.DMA((parts,)),
            pltpu.SemaphoreType.DMA((parts, 2)),
        ],
        compiler_params=pltpu.CompilerParams(collective_id=0, has_side_effects=True, vmem_limit_bytes=48 * 2**20),
    )(
        x,
        span_weights,
        wall_filter,
        prev_state.transpose(1, 0, 2),
        time_scale,
        mean_velocity.reshape(1, width),
        lund_diag,
        lund_off,
    )
    velocity = velocity.reshape(planes, kinds, rows, width).transpose(2, 0, 1, 3)
    return velocity, state.transpose(1, 0, 2)


def from_partner(value, axis, bit):
    return lax.ppermute(value, axis, [(i, i ^ 1 << bit) for i in range(lax.axis_size(axis))])


def band_matrix(taps, height):
    reach = taps.shape[0]
    padded = jnp.concatenate([taps, jnp.zeros((height,), taps.dtype)])
    length = reach + height
    tiled = jnp.tile(padded, height)[: height * (length - 1)]
    return tiled.reshape(height, length - 1)


def butterfly(held, forward):
    count = lax.axis_size("span")
    device = lax.axis_index("span")
    levels = count.bit_length() - 1
    for level in range(levels - 1, -1, -1):
        groups, inner_first, targets, inner_last = held.shape
        halves = held.reshape(groups, inner_first, 2, targets // 2, inner_last)
        lower = halves[:, :, 0]
        higher = halves[:, :, 1]
        upper = device >> level & 1 == 1
        kept = jnp.where(upper, higher, lower)
        given = jnp.where(upper, lower, higher)
        if forward:
            taken = from_partner(given, "span", level)
        else:
            taken = from_partner(given, "span", level)
        first = jnp.where(upper, taken, kept)
        second = jnp.where(upper, kept, taken)
        held = jnp.stack([first, second], axis=1).reshape(
            groups * 2, inner_first, targets // 2, inner_last
        )
    return held


def body(
    random_slabs,
    span_weights,
    wall_filter,
    prev_state,
    time_scale,
    mean_velocity,
    lund_diag,
    lund_off,
):
    rows = random_slabs.shape[0]
    planes = random_slabs.shape[1]
    width = random_slabs.shape[3]
    columns = planes * 3 * width
    half = (span_weights.shape[0] - 1) // 2
    if fits(lax.axis_size("span"), rows, planes * 3, width, half, LANES):
        return exchanged(
            random_slabs,
            span_weights,
            wall_filter,
            prev_state,
            time_scale,
            mean_velocity,
            lund_diag,
            lund_off,
        )
    flat = random_slabs.reshape(rows, columns)
    scaling = jnp.sqrt(jnp.sum(span_weights * span_weights))
    taps = (span_weights / scaling).astype(jnp.bfloat16)
    reach = (span_weights.shape[0] - 1) // 2
    count = lax.axis_size("span")
    slim = columns // count
    held = butterfly(flat.reshape(1, rows, count, slim), True)
    total = rows * count
    whole = held.reshape(total, slim)
    height = min(512, total)
    matrix = band_matrix(taps, height)
    wrapped = jnp.concatenate([whole[total - reach :], whole, whole[:reach]], axis=0)

    def one_block(start):
        window = lax.dynamic_slice_in_dim(wrapped, start, height + 2 * reach, 0)
        return jnp.dot(matrix, window, preferred_element_type=jnp.float32)

    starts = jnp.arange(total // height) * height
    summed_cols = lax.map(one_block, starts).reshape(total, slim)
    rounded = summed_cols.astype(jnp.bfloat16)
    returned = butterfly(rounded.reshape(1, 1, count, rows * slim), False)
    spanned = returned.reshape(count, rows, slim).transpose(1, 0, 2).reshape(rows, planes, 3, width)
    filtered = lax.dot_general(
        spanned, wall_filter, (((3,), (1,)), ((), ())), preferred_element_type=jnp.float32
    )
    decay = jnp.exp(-jnp.pi / (2.0 * time_scale))
    inject = jnp.sqrt(1.0 - jnp.exp(-jnp.pi / time_scale))
    state = prev_state
    outputs = []
    for plane in range(planes):
        state = decay * state + inject * filtered[:, plane]
        along = state[:, 0]
        normal = state[:, 1]
        spanwise = state[:, 2]
        first = mean_velocity + lund_diag[0] * along
        second = lund_off[0] * along + lund_diag[1] * normal
        third = lund_off[1] * along + lund_off[2] * normal + lund_diag[2] * spanwise
        outputs.append(jnp.stack([first, second, third], axis=1).astype(jnp.bfloat16))
    velocity = jnp.stack(outputs, axis=1)
    return (velocity, state)


def solution(mesh):
    placed = (P("span", None, None, None), P(), P(), P("span", None, None), P(), P(), P(), P())
    return jax.shard_map(
        body,
        mesh=mesh,
        in_specs=placed,
        out_specs=(P("span", None, None, None), P("span", None, None)),
        check_vma=False,
    )
```
